32 devices in a mesh: groups: 2 (over x), req: 8 (over z, y), head: 2 (over core).
Axes of the slice: x: 2, y: 2, z: 4, core: 2. Of those that a mesh axis runs over, the one named last changes fastest.
Arguments:
- queries: bfloat16 [16, 8192], P(('groups', 'req')), parts along dimension 0, may hold values from -120 to 120
- prefix_cache: bfloat16 [16, 4096, 2048], P(('groups', 'req'), 'head'), parts along dimension 0, may hold values from -4.1 to 4.1
- paged_pool_cache: bfloat16 [2, 256, 16, 2048], P('head', ('groups', 'req')), parts along dimension 1, may hold values from -4 to 4
- block_table: int32 [2, 16, 16], P('head', ('groups', 'req')), parts along dimension 1, may hold values from 0 to 15
- lengths: int32 [2, 16], P('head', ('groups', 'req')), parts along dimension 1, may hold values from 1 to 256
- owner: int32 [2], P('groups'), parts along dimension 0, may hold values from 0 to 7
Outputs:
- attended: bfloat16 [16, 8192], P(('groups', 'req')), parts along dimension 0
The draws below stay inside these ranges and needn't reach their ends.
There are 2 independent parts, one for each index of `groups`. The reference program is written for one: setup_inputs(seed, part) draws one part's arguments, and reference() takes and returns one part's arrays. A program takes and returns all parts, laid end to end along the dimension named above; each array names one. Nothing has to cross between parts.
Inputs may be any that keep to these rules, and one draw needn't show every extreme that they name: `block_table`: entries index the pages that the request's own rank holds, as the steps say.
All inputs are finite; a program needn't handle non-finite values.
Results may differ from the reference program's by a relative error of at most 0.014.
Values may be sent and summed in bfloat16 or wider, within the bound.
A program may use at most 64 MiB of HBM per device.

```python
import jax
import jax.numpy as jnp
from jax import lax

QUERY_HEADS = 64
KEY_VALUE_HEADS = 8
HEAD_SIZE = 128
REQUESTS_LOCAL = 1
MAXB = 16
PAGE_POSITIONS = 16
REQUESTS = 8
PREFIX_LENGTH = 4096
PAGES_DEV = 16
POOL_PAGES = 128
N_REQ = 8
N_HEAD = 2


def draw_queries(key, part):
    base = jnp.clip(jax.random.normal(jax.random.fold_in(key, 11), (REQUESTS, QUERY_HEADS * HEAD_SIZE), jnp.float32), -4.0, 4.0)
    return base.astype(jnp.bfloat16)


def draw_prefix_cache(key, part):
    array_shape = (N_REQ, PREFIX_LENGTH, 2 * KEY_VALUE_HEADS * HEAD_SIZE)
    base = jnp.clip(jax.random.normal(jax.random.fold_in(key, 21), array_shape, jnp.float32), -4.0, 4.0)
    return base.astype(jnp.bfloat16)


def touch_ends(values, key, low, largest):
    extent = values.shape
    spot = [jax.random.randint(jax.random.fold_in(key, axis), (), 0, extent[axis]) for axis in range(len(extent))]
    values = values.at[tuple(spot)].set(low)
    longest = extent.index(max(extent))
    spot[longest] = (spot[longest] + 1) % extent[longest]
    return values.at[tuple(spot)].set(largest)


def level_of(stream_key, dims, split, least, top_value):
    loudness = 1.0
    for dim, parts in split:
        steps = jax.random.uniform(jax.random.fold_in(jax.random.fold_in(stream_key, 6), dim), (parts,), jnp.float32, least / len(split), top_value / len(split))
        loudness = loudness * jnp.repeat(jnp.exp(steps), dims[dim] // parts).reshape((-1,) + (1,) * (len(dims) - 1 - dim))
    return loudness


def scatter_about(rng, extent, spread, most, split=(), kind=jnp.bfloat16):
    values = spread * jax.random.normal(rng, extent, jnp.float32)
    if split:
        values = values * level_of(rng, extent, split, -0.22, 0.18)
    return jnp.clip(values, -most, most).astype(kind)


def setup_inputs(seed: int = 0, part: int = 0) -> dict:
    key_list = jax.random.split(jax.random.key(seed), 7)
    part_splits = jax.random.split(jax.random.fold_in(key_list[6], part), 7)
    queries = draw_queries(jax.random.fold_in(jax.random.fold_in(key_list[6], part), 71), part)
    prefix_cache = draw_prefix_cache(jax.random.fold_in(jax.random.fold_in(key_list[6], part), 71), part)
    paged_pool_cache = scatter_about(part_splits[2], (N_HEAD, POOL_PAGES, PAGE_POSITIONS, 2 * KEY_VALUE_HEADS * HEAD_SIZE), 1.0, 4.0, ((0, 2), (1, 8)))
    block_table = touch_ends(jax.random.randint(part_splits[3], (N_HEAD, REQUESTS, MAXB), 0, PAGES_DEV), jax.random.fold_in(part_splits[3], 1), 0, PAGES_DEV - 1).astype(jnp.int32)
    lengths = touch_ends(jax.random.randint(part_splits[4], (N_HEAD, REQUESTS), 1, MAXB * PAGE_POSITIONS + 1), jax.random.fold_in(part_splits[4], 1), 1, MAXB * PAGE_POSITIONS).astype(jnp.int32)
    owner = jax.random.randint(part_splits[5], (1,), 0, N_REQ).astype(jnp.int32)
    return dict(queries=queries, prefix_cache=prefix_cache, paged_pool_cache=paged_pool_cache, block_table=block_table, lengths=lengths, owner=owner)


def reference(queries, prefix_cache, paged_pool_cache, block_table, lengths, owner):
    width_total = KEY_VALUE_HEADS * HEAD_SIZE
    queries_per_group = QUERY_HEADS // KEY_VALUE_HEADS
    scale = 1.0 / (HEAD_SIZE ** 0.5)
    prefix_tensor = lax.dynamic_index_in_dim(prefix_cache, owner[0], 0, keepdims=False)
    prefix_keys = prefix_tensor[:, :width_total].reshape(PREFIX_LENGTH, KEY_VALUE_HEADS, HEAD_SIZE).astype(jnp.float32)
    prefix_values = prefix_tensor[:, width_total:].reshape(PREFIX_LENGTH, KEY_VALUE_HEADS, HEAD_SIZE).astype(jnp.float32)
    rank_ids = jnp.arange(N_REQ, dtype=jnp.int32)
    query_block_rows = queries.reshape(N_REQ, REQUESTS_LOCAL, KEY_VALUE_HEADS, queries_per_group, HEAD_SIZE)
    table_blocks = jnp.transpose(block_table.reshape(N_HEAD, N_REQ, REQUESTS_LOCAL, MAXB), (1, 0, 2, 3))
    length_blocks = jnp.transpose(lengths.reshape(N_HEAD, N_REQ, REQUESTS_LOCAL), (1, 0, 2))
    halves = jnp.arange(N_HEAD, dtype=jnp.int32)[:, None, None]
    position = jnp.arange(MAXB * PAGE_POSITIONS, dtype=jnp.int32)

    def one_rank(items):
        query, table, length, rank = items
        pages = (rank * PAGES_DEV + table).astype(jnp.int32)
        gathered_pages = paged_pool_cache[halves, pages]
        gathered_pages = jnp.transpose(gathered_pages, (1, 0, 2, 3, 4)).reshape(REQUESTS_LOCAL, N_HEAD * MAXB * PAGE_POSITIONS, 2 * width_total)
        gathered_pages = gathered_pages.astype(jnp.float32)
        suffix_keys = gathered_pages[:, :, :width_total].reshape(REQUESTS_LOCAL, -1, KEY_VALUE_HEADS, HEAD_SIZE)
        suffix_values = gathered_pages[:, :, width_total:].reshape(REQUESTS_LOCAL, -1, KEY_VALUE_HEADS, HEAD_SIZE)
        live = position[None, None, :] < length[:, :, None]
        live = jnp.transpose(live, (1, 0, 2)).reshape(REQUESTS_LOCAL, -1)
        page_lookup = query.astype(jnp.float32)
        pre = jnp.einsum('rkgd,tkd->rkgt', page_lookup, prefix_keys) * scale
        suf = jnp.einsum('rkgd,rtkd->rkgt', page_lookup, suffix_keys) * scale
        suf = jnp.where(live[:, None, None, :], suf, -jnp.inf)
        top = jnp.maximum(jnp.max(pre, axis=-1), jnp.max(suf, axis=-1))
        pre_w = lax.optimization_barrier(jnp.exp(pre - top[..., None]).astype(jnp.bfloat16)).astype(jnp.float32)
        suf_w = lax.optimization_barrier(jnp.exp(suf - top[..., None]).astype(jnp.bfloat16)).astype(jnp.float32)
        total = jnp.sum(pre_w, axis=-1) + jnp.sum(suf_w, axis=-1)
        summed = jnp.einsum('rkgt,tkd->rkgd', pre_w, prefix_values) + jnp.einsum('rkgt,rtkd->rkgd', suf_w, suffix_values)
        result = (summed / total[..., None]).reshape(REQUESTS_LOCAL, QUERY_HEADS * HEAD_SIZE)
        return result.astype(jnp.bfloat16)

    outputs = lax.map(one_rank, (query_block_rows, table_blocks, length_blocks, rank_ids))
    return outputs.reshape(REQUESTS, QUERY_HEADS * HEAD_SIZE)
```

```python
import functools
import math

import jax
import jax.numpy as jnp
from jax import lax
from jax.experimental import pallas as pl
from jax.experimental.pallas import tpu as pltpu
from jax.sharding import PartitionSpec as P

QUERY_HEADS = 64
KEY_VALUE_HEADS = 8
HEAD_SIZE = 128
GROUP = QUERY_HEADS // KEY_VALUE_HEADS
PAIRS = KEY_VALUE_HEADS // 2
WIDTH = KEY_VALUE_HEADS * HEAD_SIZE
DUO = 2 * HEAD_SIZE
ROWS = 2 * GROUP
RATE = HEAD_SIZE ** (-0.5) / math.log(2.0)
MESH = pl.DeviceIdType.MESH


def each(first, last, step):
    if last - first <= 8:
        for index in range(first, last):
            step(index)
    else:
        lax.fori_loop(first, last, lambda index, carry: (step(index), carry)[1], 0)


def second_head(shape):
    return lax.rem(lax.broadcasted_iota(jnp.int32, shape, 0), ROWS) >= GROUP


def block_diagonal(block):
    odd = second_head(block.shape)
    zero = jnp.zeros_like(block)
    return jnp.concatenate([jnp.where(odd, zero, block), jnp.where(odd, block, zero)], axis=1)


def contract_last(left, right):
    return lax.dot_general(left, right, (((1,), (1,)), ((), ())), preferred_element_type=jnp.float32)


def own_columns(product):
    left = product[:, :HEAD_SIZE]
    return jnp.where(second_head(left.shape), product[:, HEAD_SIZE:], left)


def kernel(
    n, batch, queries, prefix, pool, table, lengths, owner, out,
    q_in, q_rows, q_own, q_all, keys, values, pages, table_s, length_s, owner_s,
    part_out, stat_out, part_in, stat_in, suffix, suffix_stat, halves, result,
    load_sem, page_sem, key_sem, value_sem, q_send, q_recv, p_send, p_recv, s_send, s_recv, h_send, h_recv,
):
    group = lax.axis_index("groups")
    me = lax.axis_index("req")
    half = lax.axis_index("head")

    q_load = pltpu.make_async_copy(queries, q_in, load_sem.at[0])
    q_load.start()
    small = [
        pltpu.make_async_copy(table, table_s, load_sem.at[1]),
        pltpu.make_async_copy(lengths, length_s, load_sem.at[2]),
        pltpu.make_async_copy(owner, owner_s, load_sem.at[3]),
    ]
    for copy in small:
        copy.start()
    barrier = pltpu.get_barrier_semaphore()

    def greet(step):
        peer = lax.rem(me + step, n)
        pl.semaphore_signal(barrier, inc=1, device_id=(group, peer, half), device_id_type=MESH)

    each(1, n, greet)
    pl.semaphore_signal(barrier, inc=1, device_id=(group, me, 1 - half), device_id_type=MESH)
    page_load = pltpu.make_async_copy(pool.at[0], pages, page_sem)
    page_load.start()
    loads = []
    for pair in range(PAIRS):
        key_load = pltpu.make_async_copy(prefix.at[0, :, pl.ds(pair * DUO, DUO)], keys.at[pair], key_sem.at[pair])
        value_load = pltpu.make_async_copy(
            prefix.at[0, :, pl.ds(WIDTH + pair * DUO, DUO)], values.at[pair], value_sem.at[pair]
        )
        key_load.start()
        value_load.start()
        loads.append((key_load, value_load))

    q_load.wait()
    flat = q_in[...].astype(jnp.float32)
    for head in range(QUERY_HEADS):
        q_rows[pl.ds(head, 1), :] = flat[:, head * HEAD_SIZE : (head + 1) * HEAD_SIZE]
    for pair in range(PAIRS):
        rows = q_rows[pl.ds(pair * ROWS, ROWS), :].astype(jnp.bfloat16)
        q_own[pair] = rows
        q_all[pair, me] = rows

    pl.semaphore_wait(barrier, n)

    def q_copy(pair, step):
        return pltpu.make_async_remote_copy(
            src_ref=q_own.at[pair], dst_ref=q_all.at[pair, me],
            send_sem=q_send.at[pair, step], recv_sem=q_recv.at[pair, step],
            device_id=(group, lax.rem(me + step, n), half), device_id_type=MESH,
        )

    def p_copy(pair, step):
        peer = lax.rem(me + step, n)
        return pltpu.make_async_remote_copy(
            src_ref=part_out.at[pair, peer], dst_ref=part_in.at[me, pair],
            send_sem=p_send.at[pair, step], recv_sem=p_recv.at[pair, step],
            device_id=(group, peer, half), device_id_type=MESH,
        )

    def s_copy(step):
        peer = lax.rem(me + step, n)
        return pltpu.make_async_remote_copy(
            src_ref=stat_out.at[peer], dst_ref=stat_in.at[me],
            send_sem=s_send.at[step], recv_sem=s_recv.at[step],
            device_id=(group, peer, half), device_id_type=MESH,
        )

    for pair in range(PAIRS):
        each(1, n, lambda step, pair=pair: q_copy(pair, step).start())

    for copy in small:
        copy.wait()
    page_count, page_rows = pages.shape[0], pages.shape[1]
    slots = page_count * page_rows
    spot = lax.broadcasted_iota(jnp.int32, (ROWS, slots), 1)
    page, inside = spot // page_rows, lax.rem(spot, page_rows)
    uses = jnp.zeros((ROWS, slots), jnp.float32)
    for slot in range(table_s.shape[2]):
        hit = (page == table_s[0, 0, slot]) & (inside + slot * page_rows < length_s[0, 0])
        uses += jnp.where(hit, 1.0, 0.0)
    page_load.wait()
    for pair in range(PAIRS):
        page_keys = pages[:, :, pair * DUO : (pair + 1) * DUO].reshape(slots, DUO)
        page_values = pages[:, :, WIDTH + pair * DUO : WIDTH + (pair + 1) * DUO].reshape(slots, DUO)
        scores = contract_last(block_diagonal(q_own[pair]), page_keys)
        scores = jnp.where(uses > 0.0, scores, -jnp.inf)
        top = jnp.max(scores, axis=1, keepdims=True)
        weights = jnp.exp2((scores - top) * RATE).astype(jnp.bfloat16).astype(jnp.float32) * uses
        total = jnp.sum(weights, axis=1, keepdims=True)
        summed = jnp.dot(weights.astype(jnp.bfloat16), page_values, preferred_element_type=jnp.float32)
        suffix[pair] = own_columns(summed)
        suffix_stat[pair, 0] = jnp.broadcast_to(top, (ROWS, HEAD_SIZE))
        suffix_stat[pair, 1] = jnp.broadcast_to(total, (ROWS, HEAD_SIZE))

    lane = lax.broadcasted_iota(jnp.int32, (batch, GROUP, HEAD_SIZE), 2)
    for pair in range(PAIRS):
        each(1, n, lambda step, pair=pair: q_copy(pair, step).wait_recv())
        loads[pair][0].wait()
        loads[pair][1].wait()

        def attend(index, pair=pair):
            block = pl.ds(index * batch, batch)
            rows = q_all[pair, block].reshape(batch * ROWS, HEAD_SIZE)
            scores = contract_last(block_diagonal(rows), keys[pair])
            top = jnp.max(scores, axis=1, keepdims=True)
            weights = jnp.exp2((scores - top) * RATE).astype(jnp.bfloat16)
            total = jnp.sum(weights.astype(jnp.float32), axis=1, keepdims=True)
            summed = jnp.dot(weights, values[pair], preferred_element_type=jnp.float32)
            part_out[pair, block] = own_columns(summed).reshape(batch, ROWS, HEAD_SIZE).astype(jnp.bfloat16)
            wide = (batch, 2, GROUP, HEAD_SIZE)
            tops = jnp.broadcast_to(top, (batch * ROWS, HEAD_SIZE)).reshape(wide)
            totals = jnp.broadcast_to(total, (batch * ROWS, HEAD_SIZE)).reshape(wide)
            stats = jnp.zeros((batch, GROUP, HEAD_SIZE), jnp.float32) if pair == 0 else stat_out[block]
            for side in range(2):
                place = 2 * (2 * pair + side)
                stats = jnp.where(lane == place, tops[:, side], stats)
                stats = jnp.where(lane == place + 1, totals[:, side], stats)
            stat_out[block] = stats

        each(0, n // batch, attend)
        each(1, n, lambda step, pair=pair: p_copy(pair, step).start())
    each(1, n, lambda step: s_copy(step).start())
    for pair in range(PAIRS):
        part_in[me, pair] = part_out[pair, me]
    stat_in[me] = stat_out[me]

    for pair in range(PAIRS):
        each(1, n, lambda step, pair=pair: p_copy(pair, step).wait_recv())
    each(1, n, lambda step: s_copy(step).wait_recv())

    root = owner_s[0]
    arrived = part_in[root]
    stats = stat_in[root]
    mine = jnp.zeros((GROUP, HEAD_SIZE), jnp.float32)
    narrow = lax.broadcasted_iota(jnp.int32, (GROUP, HEAD_SIZE), 1)
    for head in range(KEY_VALUE_HEADS):
        pair, side = head // 2, pl.ds((head % 2) * GROUP, GROUP)
        top_a = jnp.broadcast_to(stats[:, 2 * head : 2 * head + 1], (GROUP, HEAD_SIZE))
        total_a = jnp.broadcast_to(stats[:, 2 * head + 1 : 2 * head + 2], (GROUP, HEAD_SIZE))
        low = (head % 2) * GROUP
        sum_a = arrived[pair].astype(jnp.float32)[low : low + GROUP]
        top_b, total_b, sum_b = suffix_stat[pair, 0, side], suffix_stat[pair, 1, side], suffix[pair, side]
        top = jnp.maximum(top_a, top_b)
        early, later = jnp.exp2((top_a - top) * RATE), jnp.exp2((top_b - top) * RATE)
        halves[half, head] = sum_a * early + sum_b * later
        mine = jnp.where(narrow == 2 * head, top, mine)
        mine = jnp.where(narrow == 2 * head + 1, total_a * early + total_b * later, mine)
    halves[half, KEY_VALUE_HEADS] = mine
    swap = pltpu.make_async_remote_copy(
        src_ref=halves.at[half], dst_ref=halves.at[half], send_sem=h_send, recv_sem=h_recv,
        device_id=(group, me, 1 - half), device_id_type=MESH,
    )
    swap.start()
    swap.wait_recv()
    stat_a, stat_b = halves[0, KEY_VALUE_HEADS], halves[1, KEY_VALUE_HEADS]
    for head in range(KEY_VALUE_HEADS):
        full = (GROUP, HEAD_SIZE)
        top_a = jnp.broadcast_to(stat_a[:, 2 * head : 2 * head + 1], full)
        top_b = jnp.broadcast_to(stat_b[:, 2 * head : 2 * head + 1], full)
        total_a = jnp.broadcast_to(stat_a[:, 2 * head + 1 : 2 * head + 2], full)
        total_b = jnp.broadcast_to(stat_b[:, 2 * head + 1 : 2 * head + 2], full)
        top = jnp.maximum(top_a, top_b)
        early, later = jnp.exp2((top_a - top) * RATE), jnp.exp2((top_b - top) * RATE)
        summed = halves[0, head] * early + halves[1, head] * later
        result[pl.ds(head * GROUP, GROUP), :] = summed / (total_a * early + total_b * later)
    for head in range(QUERY_HEADS):
        out[:, head * HEAD_SIZE : (head + 1) * HEAD_SIZE] = result[pl.ds(head, 1), :].astype(out.dtype)

    for pair in range(PAIRS):
        each(1, n, lambda step, pair=pair: q_copy(pair, step).wait_send())
        each(1, n, lambda step, pair=pair: p_copy(pair, step).wait_send())
    each(1, n, lambda step: s_copy(step).wait_send())
    swap.wait_send()


def body(n, queries, prefix_cache, paged_pool_cache, block_table, lengths, owner):
    length = prefix_cache.shape[1]
    batch = math.gcd(n, 8)
    anywhere = pl.BlockSpec(memory_space=pl.ANY)
    bf16, f32 = jnp.bfloat16, jnp.float32
    dma = pltpu.SemaphoreType.DMA
    return pl.pallas_call(
        functools.partial(kernel, n, batch),
        out_shape=jax.ShapeDtypeStruct(queries.shape, bf16),
        in_specs=[anywhere] * 6,
        out_specs=pl.BlockSpec(memory_space=pltpu.VMEM),
        scratch_shapes=[
            pltpu.VMEM(queries.shape, bf16),
            pltpu.VMEM((QUERY_HEADS, HEAD_SIZE), f32),
            pltpu.VMEM((PAIRS, ROWS, HEAD_SIZE), bf16),
            pltpu.VMEM((PAIRS, n, ROWS, HEAD_SIZE), bf16),
            pltpu.VMEM((PAIRS, length, DUO), bf16),
            pltpu.VMEM((PAIRS, length, DUO), bf16),
            pltpu.VMEM(paged_pool_cache.shape[1:], bf16),
            pltpu.SMEM(block_table.shape, jnp.int32),
            pltpu.SMEM(lengths.shape, jnp.int32),
            pltpu.SMEM(owner.shape, jnp.int32),
            pltpu.VMEM((PAIRS, n, ROWS, HEAD_SIZE), bf16),
            pltpu.VMEM((n, GROUP, HEAD_SIZE), f32),
            pltpu.VMEM((n, PAIRS, ROWS, HEAD_SIZE), bf16),
            pltpu.VMEM((n, GROUP, HEAD_SIZE), f32),
            pltpu.VMEM((PAIRS, ROWS, HEAD_SIZE), f32),
            pltpu.VMEM((PAIRS, 2, ROWS, HEAD_SIZE), f32),
            pltpu.VMEM((2, KEY_VALUE_HEADS + 1, GROUP, HEAD_SIZE), f32),
            pltpu.VMEM((QUERY_HEADS, HEAD_SIZE), f32),
            dma((4,)),
            dma,
            dma((PAIRS,)),
            dma((PAIRS,)),
            dma((PAIRS, n)),
            dma((PAIRS, n)),
            dma((PAIRS, n)),
            dma((PAIRS, n)),
            dma((n,)),
            dma((n,)),
            dma,
            dma,
        ],
        compiler_params=pltpu.CompilerParams(collective_id=0, has_side_effects=True),
    )(queries, prefix_cache, paged_pool_cache, block_table, lengths, owner)


def solution(mesh):
    placed = (
        P(("groups", "req"), None),
        P(("groups", "req"), "head", None),
        P("head", ("groups", "req"), None, None),
        P("head", ("groups", "req"), None),
        P("head", ("groups", "req")),
        P("groups"),
    )
    return jax.shard_map(
        functools.partial(body, mesh.shape["req"]),
        mesh=mesh, in_specs=placed, out_specs=P(("groups", "req"), None), check_vma=False,
    )
```
